32 devices in a mesh: grp: 2 (over x), blk: 16 (over z, y, core).
Axes of the slice: x: 2, y: 2, z: 4, core: 2. Of those that a mesh axis runs over, the one named last changes fastest.
Arguments:
- atoms: bfloat16 [16384, 512], P(('grp', 'blk')), parts along dimension 0, may hold values from -8 to 8
- edge_mask: int32 [32, 5, 512, 512], P(('grp', 'blk')), parts along dimension 0, may hold values from 0 to 1
- norm_gain: float32 [512], replicated, may hold values from 0.25 to 1.75
- w_query: bfloat16 [512, 512], replicated, may hold values from -3 to 3
- w_key: bfloat16 [512, 512], replicated, may hold values from -3 to 3
- w_value: bfloat16 [512, 512], replicated, may hold values from -0.25 to 0.25
- w_out: bfloat16 [512, 512], replicated, may hold values from -0.25 to 0.25
- bn_gain: float32 [512], replicated, may hold values from 0.25 to 1.75
- bn_shift: float32 [512], replicated, may hold values from -3 to 3
- w_up: bfloat16 [512, 1024], replicated, may hold values from -0.25 to 0.25
- w_down: bfloat16 [1024, 512], replicated, may hold values from -0.1875 to 0.1875
Outputs:
- updated: bfloat16 [16384, 512], P(('grp', 'blk')), parts along dimension 0
The draws below stay inside these ranges and needn't reach their ends.
There are 2 independent parts, one for each index of `grp`. The reference program is written for one: setup_inputs(seed, part) draws one part's arguments, and reference() takes and returns one part's arrays. A program takes and returns all parts, laid end to end along the dimension named above; an argument that names none is the same for every part. Nothing has to cross between parts.
All inputs are finite; a program needn't handle non-finite values.
Results may differ from the reference program's by a relative error of at most 0.01.
The reference program's roundings to bfloat16 on the way (of `normed`, `query`, `weight`, `mixed`, `batched` and `hidden`) count: a program that leaves them out, or rounds other values in their place, can miss the bound.
Values may be sent and summed in bfloat16 or wider, within the bound.
No kernel may reach another device: no remote copies, remote signals or barrier semaphores. Data moves between devices by JAX's collectives and lax.ppermute only.
A program may use at most 128 MiB of HBM per device.

```python
import jax
import jax.numpy as jnp
from jax import lax

D = 512
HEADS = 8
HEAD_DIM = 64
FF = 1024
REACH = 2
TILE = 512
ATOMS = 8192


def draw_atoms(key, part):
    key_base = jax.random.fold_in(key, 11)
    key_one, key_two, key_three, key_four = jax.random.split(key_base, 4)
    ntiles = ATOMS // TILE
    tile_ids = (jnp.arange(ATOMS) // TILE).astype(jnp.int32)
    tile_index = tile_ids.astype(jnp.float32)
    rising = (1.0 + 2.0 * tile_index / (ntiles - 1))[:, None]
    parity = (1 - 2 * (tile_ids % 2)).astype(jnp.float32)[:, None]
    row_scale = jnp.exp(jax.random.uniform(key_two, (ATOMS, 1), jnp.float32, -0.69, 0.69))
    noise = jnp.clip(jax.random.normal(key_one, (ATOMS, D), jnp.float32), -6.0, 6.0)
    feature_mean = jnp.clip(jax.random.normal(key_three, (1, D), jnp.float32), -3.0, 3.0)
    bulk = noise * row_scale * rising + feature_mean * rising
    alternate = jnp.clip(jax.random.normal(key_four, (1, D), jnp.float32), -3.0, 3.0)
    return (0.1 * (bulk + alternate * parity)).astype(jnp.bfloat16)


def projection_draw(key, salt):
    base = jax.random.normal(jax.random.fold_in(key, salt), (D, D), jnp.float32)
    base = jnp.clip(base, -4.0, 4.0) * D ** (-0.5)
    return base.astype(jnp.bfloat16)


def draw_w_query(key, part):
    return projection_draw(key, 21)


def draw_w_key(key, part):
    return projection_draw(key, 22)


def draw_edge_mask(key, part):
    ntiles = ATOMS // TILE
    widths = 2 * REACH + 1
    key_base = jax.random.fold_in(key, 31)
    key_one, key_two, key_three = jax.random.split(key_base, 3)
    cut_level = jax.random.randint(key_one, (ntiles, widths, 1, 1), 0, 12)
    own_level = jax.random.randint(key_two, (ntiles, widths, 1, 1), 6, 24)
    offset = jnp.arange(widths).reshape(1, widths, 1, 1)
    level = jnp.where(offset == REACH, own_level, cut_level)
    draws = jax.random.randint(key_three, (ntiles, widths, TILE, TILE), 0, 64)
    return (draws < level).astype(jnp.int32)


def centred(key, extent, scale, reach, dtype=jnp.bfloat16):
    values = scale * jax.random.normal(key, extent, jnp.float32)
    return jnp.clip(values, min=-reach, max=reach).astype(dtype)


def setup_inputs(seed: int = 0, part: int = 0) -> dict:
    splits = jax.random.split(jax.random.key(seed), 12)
    part_keys = jax.random.split(jax.random.fold_in(splits[11], part), 12)
    return {
        "atoms": draw_atoms(jax.random.fold_in(jax.random.fold_in(splits[11], part), 71), part),
        "edge_mask": draw_edge_mask(jax.random.fold_in(jax.random.fold_in(splits[11], part), 71), part),
        "norm_gain": jnp.clip(1.0 + 0.15 * jax.random.normal(splits[2], (D,), jnp.float32), 0.25, 1.75),
        "w_query": draw_w_query(jax.random.fold_in(splits[11], 71), part),
        "w_key": draw_w_key(jax.random.fold_in(splits[11], 71), part),
        "w_value": centred(splits[5], (D, D), D ** -0.5, 0.25),
        "w_out": centred(splits[6], (D, D), D ** -0.5, 0.25),
        "bn_gain": jnp.clip(1.0 + 0.15 * jax.random.normal(splits[7], (D,), jnp.float32), 0.25, 1.75),
        "bn_shift": centred(splits[8], (D,), 0.5, 3.0, jnp.float32),
        "w_up": centred(splits[9], (D, FF), D ** -0.5, 0.25),
        "w_down": centred(splits[10], (FF, D), FF ** -0.5, 0.1875),
    }


def reference(atoms, edge_mask, norm_gain, w_query, w_key, w_value, w_out, bn_gain, bn_shift, w_up, w_down):
    ntiles = ATOMS // TILE
    widths = 2 * REACH + 1
    scale = HEAD_DIM ** (-0.5)
    xfull = atoms.astype(jnp.float32)
    normed = (xfull * lax.rsqrt(lax.optimization_barrier(jnp.mean(xfull * xfull, axis=-1, keepdims=True)) + 1e-06) * norm_gain).astype(jnp.bfloat16)
    query = jnp.dot(normed, w_query, preferred_element_type=jnp.float32).astype(jnp.bfloat16)
    keys = jnp.dot(normed, w_key, preferred_element_type=jnp.float32).astype(jnp.bfloat16)
    values = jnp.dot(normed, w_value, preferred_element_type=jnp.float32).astype(jnp.bfloat16)
    q_tiles = query.reshape(ntiles, TILE, HEADS, HEAD_DIM)
    k_tiles = keys.reshape(ntiles, TILE, HEADS, HEAD_DIM)
    v_tiles = values.reshape(ntiles, TILE, HEADS, HEAD_DIM)
    k_near = jnp.stack([jnp.roll(k_tiles, -(o - REACH), axis=0) for o in range(widths)], axis=1).reshape(ntiles, widths * TILE, HEADS, HEAD_DIM)
    v_near = jnp.stack([jnp.roll(v_tiles, -(o - REACH), axis=0) for o in range(widths)], axis=1).reshape(ntiles, widths * TILE, HEADS, HEAD_DIM)
    rows = lax.broadcasted_iota(jnp.int32, (TILE, widths, TILE), 0)
    cols = lax.broadcasted_iota(jnp.int32, (TILE, widths, TILE), 2)
    block = lax.broadcasted_iota(jnp.int32, (TILE, widths, TILE), 1)
    selfmask = ((rows == cols) & (block == REACH)).reshape(TILE, widths * TILE)

    def one_tile(pieces):
        qpart, kpart, vpart, mpart = pieces
        allowed = (jnp.transpose(mpart, (1, 0, 2)).reshape(TILE, widths * TILE) > 0) | selfmask
        score = jnp.einsum('qhd,khd->hqk', qpart.astype(jnp.float32), kpart.astype(jnp.float32)) * scale
        score = jnp.where(allowed[None], score, -1e+30)
        top = lax.optimization_barrier(jnp.max(score, axis=-1, keepdims=True))
        expo = jnp.exp(score - top)
        total = lax.optimization_barrier(jnp.sum(expo, axis=-1))
        weight = expo.astype(jnp.bfloat16)
        summed = jnp.einsum('hqk,khd->qhd', weight.astype(jnp.float32), vpart.astype(jnp.float32))
        return (summed / jnp.transpose(total)[:, :, None]).reshape(TILE, D).astype(jnp.bfloat16)
    mixed = lax.map(one_tile, (q_tiles, k_near, v_near, edge_mask)).reshape(ATOMS, D)
    after = xfull + jnp.dot(mixed, w_out, preferred_element_type=jnp.float32)
    mean = lax.optimization_barrier(jnp.mean(after, axis=0))
    var = lax.optimization_barrier(jnp.mean((after - mean) ** 2, axis=0))
    batched = ((after - mean) * lax.rsqrt(var + 1e-05) * bn_gain + bn_shift).astype(jnp.bfloat16)
    hidden = jax.nn.gelu(jnp.dot(batched, w_up, preferred_element_type=jnp.float32), approximate=True).astype(jnp.bfloat16)
    return (after + jnp.dot(hidden, w_down, preferred_element_type=jnp.float32)).astype(jnp.bfloat16)
```

```python
import functools

import jax
import jax.numpy as jnp
from jax import lax
from jax.experimental import pallas as pl
from jax.experimental.pallas import tpu as pltpu
from jax.sharding import PartitionSpec as P

HEADS = 8
HEAD_DIM = 64
REACH = 2
PAIR = 2 * HEAD_DIM
ONES = 16
BLOCKED = -1e30
LOG2E = 1.4426950408889634
F32 = jnp.float32
BF16 = jnp.bfloat16


def moved(value, axis, target):
    count = lax.axis_size(axis)
    pairs = [(source, target(source) % count) for source in range(count)]
    return lax.ppermute(value, axis, pairs)


def normalised(rows, gain):
    rows = rows.astype(F32)
    scale = lax.rsqrt(jnp.mean(rows * rows, axis=-1, keepdims=True) + 1e-06)
    return (rows * scale * gain).astype(BF16)


def fill_keys(normed, w_key, w_value, keys_ref, values_ref):
    tile = normed.shape[0]
    keys = jnp.dot(normed, w_key, preferred_element_type=F32).astype(BF16)
    for pair in range(HEADS // 2):
        keys_ref[pair] = keys[:, pair * PAIR : (pair + 1) * PAIR]
    values = jnp.dot(normed, w_value, preferred_element_type=F32).astype(BF16)
    values_t = jnp.transpose(values)
    for head in range(HEADS):
        values_ref[head, :HEAD_DIM, :] = values_t[head * HEAD_DIM : (head + 1) * HEAD_DIM]
        values_ref[head, HEAD_DIM:, :] = jnp.ones((ONES, tile), BF16)


def fill_bias(mask, own, bias_ref):
    tile = mask.shape[0]
    allowed = mask > 0
    if own:
        rows = lax.broadcasted_iota(jnp.int32, (tile, tile), 0)
        cols = lax.broadcasted_iota(jnp.int32, (tile, tile), 1)
        allowed = allowed | (rows == cols)
    bias = jnp.where(allowed, 0.0, BLOCKED).astype(BF16)
    bias_ref[...] = jnp.transpose(bias).astype(F32)


def attend(first, query_ref, keys_ref, values_ref, bias_ref, top_ref, sum_ref, chunk):
    tile = bias_ref.shape[0]

    def one_head(head, carry):
        keys = keys_ref[head // 2]
        for start in range(0, tile, chunk):
            cols = pl.ds(start, chunk)
            score = jnp.dot(keys, query_ref[head, :, cols], preferred_element_type=F32)
            score = score + bias_ref[:, cols]
            top = jnp.max(score, axis=0, keepdims=True)
            if not first:
                old = top_ref[head, :, cols]
                top = jnp.maximum(old, top)
                factor = jnp.exp2((old - top) * LOG2E)
            weight = jnp.exp2((score - top) * LOG2E).astype(BF16)
            product = jnp.dot(values_ref[head], weight, preferred_element_type=F32)
            if not first:
                product = sum_ref[head, :, cols] * factor + product
            top_ref[head, :, cols] = top
            sum_ref[head, :, cols] = product
        return carry

    lax.fori_loop(0, HEADS, one_head, 0)


def first_kernel(
    which_ref, own_ref, near_ref, mask_own, mask_near, gain, w_query, w_key, w_value,
    query_ref, top_ref, sum_ref, keys_ref, values_ref, bias_ref,
    *, chunk,
):
    normed = normalised(own_ref[...], gain[...])
    query = jnp.dot(normed, w_query[...], preferred_element_type=F32).astype(BF16)
    query_t = jnp.transpose(query * jnp.asarray(HEAD_DIM ** (-0.5), BF16))
    tile = query_t.shape[1]
    for head in range(HEADS):
        half = (head % 2) * HEAD_DIM
        query_ref[head, half : half + HEAD_DIM, :] = query_t[
            head * HEAD_DIM : (head + 1) * HEAD_DIM
        ]
        query_ref[head, HEAD_DIM - half : PAIR - half, :] = jnp.zeros((HEAD_DIM, tile), BF16)
    fill_bias(mask_own[0, 0], True, bias_ref)
    fill_keys(normed, w_key[...], w_value[...], keys_ref, values_ref)
    attend(True, query_ref, keys_ref, values_ref, bias_ref, top_ref, sum_ref, chunk)
    normed = normalised(near_ref[...], gain[...])
    fill_bias(mask_near[0, 0], False, bias_ref)
    fill_keys(normed, w_key[...], w_value[...], keys_ref, values_ref)
    attend(False, query_ref, keys_ref, values_ref, bias_ref, top_ref, sum_ref, chunk)


def middle_kernel(
    which_ref, one_ref, two_ref, mask_one, mask_two, gain, w_key, w_value, query_ref,
    top_in, sum_in, top_ref, sum_ref, keys_ref, values_ref, bias_ref,
    *, chunk,
):
    top_ref[...] = top_in[...]
    sum_ref[...] = sum_in[...]
    for rows_ref, mask_ref in ((one_ref, mask_one), (two_ref, mask_two)):
        normed = normalised(rows_ref[...], gain[...])
        fill_bias(mask_ref[0, 0], False, bias_ref)
        fill_keys(normed, w_key[...], w_value[...], keys_ref, values_ref)
        attend(False, query_ref, keys_ref, values_ref, bias_ref, top_ref, sum_ref, chunk)


def last_kernel(
    which_ref, far_ref, mask_far, gain, w_key, w_value, query_ref, top_in, sum_in,
    own_ref, w_out, after_ref, stats_ref, keys_ref, values_ref, bias_ref, top_ref, sum_ref,
    *, chunk,
):
    top_ref[...] = top_in[...]
    sum_ref[...] = sum_in[...]
    normed = normalised(far_ref[...], gain[...])
    fill_bias(mask_far[0, 0], False, bias_ref)
    fill_keys(normed, w_key[...], w_value[...], keys_ref, values_ref)
    attend(False, query_ref, keys_ref, values_ref, bias_ref, top_ref, sum_ref, chunk)
    mixed_t = jnp.concatenate(
        [
            (sum_ref[head, :HEAD_DIM, :] / sum_ref[head, HEAD_DIM : HEAD_DIM + 1, :]).astype(BF16)
            for head in range(HEADS)
        ],
        axis=0,
    )
    mixed = jnp.transpose(mixed_t)
    after = own_ref[...].astype(F32) + jnp.dot(mixed, w_out[...], preferred_element_type=F32)
    after_ref[...] = after
    mean = jnp.mean(after, axis=0, keepdims=True)
    centered = after - mean
    stats_ref[0:1, :] = mean
    stats_ref[1:2, :] = jnp.sum(centered * centered, axis=0, keepdims=True)


def whole(shape):
    return pl.BlockSpec(shape, lambda step, which: (0,) * len(shape))


def mask_spec(slot, tile):
    return pl.BlockSpec((1, 1, tile, tile), lambda step, which: (0, which[slot], 0, 0))


def merged(stats, rows, axis):
    count = lax.axis_size(axis)
    step = 1
    while step < count:
        other = moved(stats, axis, lambda source: source ^ step)
        gap = other[0] - stats[0]
        stats = jnp.stack(
            [
                0.5 * (stats[0] + other[0]),
                stats[1] + other[1] + gap * gap * (0.5 * rows),
            ]
        )
        rows = 2 * rows
        step = 2 * step
    return stats[0], stats[1] / rows


def body(
    atoms, edge_mask, norm_gain, w_query, w_key, w_value, w_out, bn_gain, bn_shift, w_up, w_down
):
    tile, width = atoms.shape
    chunk = tile // 2
    side = lax.axis_index("blk") % 2
    sign = 1 - 2 * side
    across = moved(atoms, "blk", lambda s: s + 1 if s % 2 else s - 1)
    mate = moved(atoms, "blk", lambda s: s ^ 1)
    far = moved(atoms, "blk", lambda s: s - 2 if s % 2 else s + 2)
    passed = moved(across, "blk", lambda s: s ^ 1)
    gain = norm_gain.reshape(1, width)

    half = jax.ShapeDtypeStruct((HEADS, PAIR, tile), BF16)
    top = jax.ShapeDtypeStruct((HEADS, 1, tile), F32)
    total = jax.ShapeDtypeStruct((HEADS, HEAD_DIM + ONES, tile), F32)
    rows_spec = whole((tile, width))
    work = [
        pltpu.VMEM((HEADS // 2, tile, PAIR), BF16),
        pltpu.VMEM((HEADS, HEAD_DIM + ONES, tile), BF16),
        pltpu.VMEM((tile, tile), F32),
    ]
    square = whole((width, width))
    gain_spec = whole((1, width))
    half_spec, top_spec, total_spec = whole(half.shape), whole(top.shape), whole(total.shape)
    params = pltpu.CompilerParams(vmem_limit_bytes=40 * 1024 * 1024)

    query_heads, tops, sums = pl.pallas_call(
        functools.partial(first_kernel, chunk=chunk),
        grid_spec=pltpu.PrefetchScalarGridSpec(
            num_scalar_prefetch=1,
            grid=(1,),
            in_specs=[rows_spec, rows_spec, mask_spec(0, tile), mask_spec(1, tile), gain_spec]
            + [square] * 3,
            out_specs=[half_spec, top_spec, total_spec],
            scratch_shapes=work,
        ),
        out_shape=[half, top, total],
        compiler_params=params,
        name="attend_first",
    )(
        jnp.stack([REACH + 0 * sign, REACH + sign]),
        atoms, mate, edge_mask, edge_mask, gain, w_query, w_key, w_value,
    )
    tops, sums = pl.pallas_call(
        functools.partial(middle_kernel, chunk=chunk),
        grid_spec=pltpu.PrefetchScalarGridSpec(
            num_scalar_prefetch=1,
            grid=(1,),
            in_specs=[rows_spec, rows_spec, mask_spec(0, tile), mask_spec(1, tile), gain_spec]
            + [square] * 2
            + [half_spec, top_spec, total_spec],
            out_specs=[top_spec, total_spec],
            scratch_shapes=work,
        ),
        out_shape=[top, total],
        compiler_params=params,
        name="attend_middle",
    )(
        jnp.stack([REACH - sign, REACH + 2 * sign]),
        across, passed, edge_mask, edge_mask, gain, w_key, w_value, query_heads, tops, sums,
    )
    after, stats = pl.pallas_call(
        functools.partial(last_kernel, chunk=chunk),
        grid_spec=pltpu.PrefetchScalarGridSpec(
            num_scalar_prefetch=1,
            grid=(1,),
            in_specs=[rows_spec, mask_spec(0, tile), gain_spec]
            + [square] * 2
            + [half_spec, top_spec, total_spec, rows_spec, square],
            out_specs=[rows_spec, whole((2, width))],
            scratch_shapes=work
            + [
                pltpu.VMEM((HEADS, 1, tile), F32),
                pltpu.VMEM((HEADS, HEAD_DIM + ONES, tile), F32),
            ],
        ),
        out_shape=[
            jax.ShapeDtypeStruct((tile, width), F32),
            jax.ShapeDtypeStruct((2, width), F32),
        ],
        compiler_params=params,
        name="attend_last",
    )(
        jnp.stack([REACH - 2 * sign]),
        far, edge_mask, gain, w_key, w_value, query_heads, tops, sums, atoms, w_out,
    )
    mean, var = merged(stats, tile, "blk")
    batched = ((after - mean) * lax.rsqrt(var + 1e-05) * bn_gain + bn_shift).astype(BF16)
    hidden = jax.nn.gelu(
        jnp.dot(batched, w_up, preferred_element_type=F32), approximate=True
    ).astype(BF16)
    return (after + jnp.dot(hidden, w_down, preferred_element_type=F32)).astype(BF16)


def solution(mesh):
    rows = P(("grp", "blk"), None)
    placed = (rows, P(("grp", "blk"), None, None, None)) + (P(),) * 9
    return jax.shard_map(body, mesh=mesh, in_specs=placed, out_specs=rows, check_vma=False)
```

```python
import functools

import jax
import jax.numpy as jnp
from jax import lax
from jax.experimental import pallas as pl
from jax.experimental.pallas import tpu as pltpu
from jax.sharding import PartitionSpec as P


HEADS = 8
HEAD_DIM = 64
REACH = 2
WIDTHS = 2 * REACH + 1
PAIR = 2 * HEAD_DIM
ROWS = 8
TOTAL = HEAD_DIM
SHIFT = HEAD_DIM + ROWS
DEPTH = HEAD_DIM + 2 * ROWS
BLOCKED = -1e30
LOG2E = 1.4426950408889634
LIMIT = 2.0**80
F32 = jnp.float32
BF16 = jnp.bfloat16


def moved(value, axis, target):
    count = lax.axis_size(axis)
    pairs = [(source, target(source) % count) for source in range(count)]
    return lax.ppermute(value, axis, pairs)


def normalised(rows, gain):
    rows = rows.astype(F32)
    scale = lax.rsqrt(jnp.mean(rows * rows, axis=-1, keepdims=True) + 1e-06)
    return (rows * scale * gain).astype(BF16)


def fill_keys(normed, w_key, keys_ref):
    keys = jnp.dot(normed, w_key, preferred_element_type=F32).astype(BF16)
    for pair in range(HEADS // 2):
        keys_ref[pair] = keys[:, pair * PAIR : (pair + 1) * PAIR]


def fill_values(normed, w_value, values_ref):
    values = jnp.dot(normed, w_value, preferred_element_type=F32).astype(BF16)
    values_t = jnp.transpose(values)
    row = lax.broadcasted_iota(jnp.int32, (2 * ROWS, values_t.shape[1]), 0)
    ones = jnp.where(row < ROWS, 1.0, 0.0).astype(BF16)
    for head in range(HEADS):
        values_ref[head, :HEAD_DIM, :] = values_t[head * HEAD_DIM : (head + 1) * HEAD_DIM]
        values_ref[head, HEAD_DIM:, :] = ones


def bias_of(mask, own):
    tile = mask.shape[0]
    allowed = mask > 0
    if own:
        rows = lax.broadcasted_iota(jnp.int32, (tile, tile), 0)
        cols = lax.broadcasted_iota(jnp.int32, (tile, tile), 1)
        allowed = allowed | (rows == cols)
    bias = jnp.where(allowed, 0.0, BLOCKED).astype(BF16)
    return jnp.transpose(bias).astype(F32)


def attend(rows, gain, w_key, w_value, query_ref, bias_ref, keep, work, old, new):
    keys_ref, values_ref = work
    slot, first = keep
    count, tile = rows.shape[0], bias_ref.shape[-1]
    ahead = 1 if 2 * count > tile else 2
    normed = normalised(rows, gain)
    fill_keys(normed, w_key, keys_ref)

    def raw(head):
        return jnp.dot(keys_ref[head // 2], query_ref[head], preferred_element_type=F32)

    def scores(product):
        return product * LOG2E + bias_ref[slot, first : first + count]

    def mix(head, weight):
        return jnp.dot(values_ref[head], weight.astype(BF16), preferred_element_type=F32)

    pending = [raw(head) for head in range(ahead)]
    fill_values(normed, w_value, values_ref)
    strayed = jnp.zeros((ROWS, tile), F32)
    for head in range(HEADS):
        if head + ahead < HEADS:
            pending.append(raw(head + ahead))
        mixed = mix(head, jnp.exp2(scores(pending.pop(0))))
        if old is not None:
            mixed = old[head] + mixed
        new[head] = mixed
        total, shift = mixed[TOTAL:SHIFT], mixed[SHIFT:]
        fits = (total <= LIMIT) & (total >= 1.0 / LIMIT) & (shift == 0.0)
        strayed = jnp.where(fits, strayed, 1.0)

    @pl.when(jnp.max(strayed) > 0.0)
    def _():
        def one_head(head, carry):
            score = scores(raw(head))
            top = jnp.max(score, axis=0, keepdims=True)
            if old is not None:
                before = old[head, SHIFT : SHIFT + 1]
                top = jnp.maximum(before, top)
            mixed = mix(head, jnp.exp2(score - top))
            if old is not None:
                mixed = old[head] * jnp.exp2(before - top) + mixed
            new[head] = mixed
            new[head, SHIFT:] = jnp.broadcast_to(top, (ROWS, tile))
            return carry

        lax.fori_loop(0, HEADS, one_head, 0)


def first_kernel(
    which_ref, own_hbm, mask_hbm, gain_ref, w_query_hbm, w_key_hbm, w_value_hbm,
    query_ref, bias_ref, sum_ref,
    own_ref, mask_ref, w_query_ref, w_key_ref, w_value_ref,
    keys_ref, values_ref, sems,
):
    fetches = [
        pltpu.make_async_copy(source, target, sems.at[index])
        for index, (source, target) in enumerate(
            [
                (own_hbm, own_ref),
                (w_query_hbm, w_query_ref),
                (w_key_hbm, w_key_ref),
                (w_value_hbm, w_value_ref),
            ]
            + [(mask_hbm.at[0, offset], mask_ref.at[offset]) for offset in range(WIDTHS)]
        )
    ]
    for fetch in fetches:
        fetch.start()
    fetches[0].wait()
    normed = normalised(own_ref[...], gain_ref[...])
    fetches[1].wait()
    query = jnp.dot(normed, w_query_ref[...], preferred_element_type=F32).astype(BF16)
    query_t = jnp.transpose(query * jnp.asarray(HEAD_DIM ** (-0.5), BF16))
    tile = query_t.shape[1]
    for head in range(HEADS):
        half = (head % 2) * HEAD_DIM
        query_ref[head, half : half + HEAD_DIM, :] = query_t[
            head * HEAD_DIM : (head + 1) * HEAD_DIM
        ]
        query_ref[head, HEAD_DIM - half : PAIR - half, :] = jnp.zeros((HEAD_DIM, tile), BF16)
    for fetch in fetches[2:]:
        fetch.wait()
    for slot in range(WIDTHS):
        bias_ref[slot] = bias_of(mask_ref[which_ref[slot]], slot == 0)
    attend(
        own_ref[...], gain_ref[...], w_key_ref[...], w_value_ref[...], query_ref, bias_ref,
        (0, 0), (keys_ref, values_ref), None, sum_ref,
    )


def next_kernel(
    rows_ref, gain_ref, w_key_ref, w_value_ref, query_ref, bias_ref, sum_in,
    sum_ref, keys_ref, values_ref, *, slot, first=0,
):
    attend(
        rows_ref[...], gain_ref[...], w_key_ref[...], w_value_ref[...], query_ref, bias_ref,
        (slot, first), (keys_ref, values_ref), sum_in, sum_ref,
    )


def last_kernel(
    rows_ref, gain_ref, w_key_ref, w_value_ref, query_ref, bias_ref, sum_in,
    own_ref, w_out_ref, after_ref, stats_ref,
    keys_ref, values_ref, sum_ref, *, slot, first,
):
    next_kernel(
        rows_ref, gain_ref, w_key_ref, w_value_ref, query_ref, bias_ref, sum_in,
        sum_ref, keys_ref, values_ref, slot=slot, first=first,
    )
    mixed_t = jnp.concatenate(
        [
            (sum_ref[head, :HEAD_DIM] * (1.0 / sum_ref[head, TOTAL : TOTAL + 1])).astype(BF16)
            for head in range(HEADS)
        ],
        axis=0,
    )
    mixed = jnp.transpose(mixed_t)
    after = own_ref[...].astype(F32) + jnp.dot(
        mixed, w_out_ref[...], preferred_element_type=F32
    )
    after_ref[...] = after
    mean = jnp.mean(after, axis=0, keepdims=True)
    centered = after - mean
    stats_ref[0:1, :] = mean
    stats_ref[1:2, :] = jnp.sum(centered * centered, axis=0, keepdims=True)


def pick_kernel(flag_ref, yes_ref, no_ref, out_ref):
    first = yes_ref.shape[0] - out_ref.shape[0]
    for value, source in ((1, yes_ref), (0, no_ref)):

        @pl.when(flag_ref[WIDTHS] == value)
        def _():
            out_ref[...] = source[first:, :]


def joined(parts, rows):
    mean = sum(part[0] for part in parts) * (1.0 / len(parts))
    spread = sum(part[1] + rows * jnp.square(part[0] - mean) for part in parts)
    return jnp.stack([mean, spread])


def merged(stats, rows, axis):
    count = lax.axis_size(axis)
    step = 1
    while step < count:
        if count % (16 * step) == 0 and step == 1:
            stats = joined([stats, moved(stats, axis, lambda s: s ^ 1)], rows)
            side = lax.axis_index(axis) % 2
            last = moved(stats, axis, lambda s: s ^ 8)
            found = [
                moved(stats, axis, lambda s, peer=peer: s ^ (8 * (s % 2) + 2 * peer))
                for peer in (1, 2, 3)
            ]
            stats = joined([jnp.where(side == 0, stats, last)] + found, 2 * rows)
            stats = joined([stats, moved(stats, axis, lambda s: s ^ 1)], 8 * rows)
            step, rows = 16, 16 * rows
        else:
            stats = joined([stats, moved(stats, axis, lambda s: s ^ step)], rows)
            step, rows = 2 * step, 2 * rows
    return stats[0], stats[1] / rows


def body(
    atoms, edge_mask, norm_gain, w_query, w_key, w_value, w_out, bn_gain, bn_shift, w_up, w_down
):
    tile, width = atoms.shape
    place = lax.axis_index("blk") % 4
    sign = 1 - 2 * (place % 2)
    inner = (place + 1) // 2 % 2
    which = jnp.stack(
        [REACH + 0 * sign, REACH + sign, REACH - sign, REACH + 2 * sign, REACH - 2 * sign, inner]
    )
    across = moved(atoms, "blk", lambda s: s + 1 if s % 2 else s - 1)
    mate = moved(atoms, "blk", lambda s: s ^ 1)
    gain = norm_gain.reshape(1, width)

    vmem = pl.BlockSpec(memory_space=pltpu.VMEM)
    hbm = pl.BlockSpec(memory_space=pltpu.HBM)
    smem = pl.BlockSpec(memory_space=pltpu.SMEM)
    state = jax.ShapeDtypeStruct((HEADS, DEPTH, tile), F32)

    def work(rows):
        return [
            pltpu.VMEM((HEADS // 2, rows, PAIR), BF16),
            pltpu.VMEM((HEADS, DEPTH, rows), BF16),
        ]


    def params(mib):
        return pltpu.CompilerParams(vmem_limit_bytes=mib * 1024 * 1024)

    cost = pl.CostEstimate(
        flops=8 * tile * tile * width, bytes_accessed=4 * tile * width, transcendentals=0
    )

    passed = moved(across, "blk", lambda s: s ^ 1)
    half = tile // 2
    far0 = moved(atoms[:half], "blk", lambda s: s - 2 if s % 2 else s + 2)
    forward = pl.pallas_call(
        pick_kernel,
        in_specs=[smem, vmem, vmem],
        out_specs=vmem,
        out_shape=jax.ShapeDtypeStruct((half, width), BF16),
        compiler_params=params(2),
        name="pick_far",
    )(which, across, atoms)
    far1 = moved(forward, "blk", lambda s: s + (2, 3, -3, -2)[s % 4])

    query_heads, bias, sums = pl.pallas_call(
        first_kernel,
        in_specs=[smem, hbm, hbm, vmem, hbm, hbm, hbm],
        out_specs=[vmem] * 3,
        out_shape=[
            jax.ShapeDtypeStruct((HEADS, PAIR, tile), BF16),
            jax.ShapeDtypeStruct((WIDTHS, tile, tile), F32),
            state,
        ],
        scratch_shapes=[
            pltpu.VMEM((tile, width), BF16),
            pltpu.VMEM((WIDTHS, tile, tile), jnp.int32),
            pltpu.VMEM((width, width), BF16),
            pltpu.VMEM((width, width), BF16),
            pltpu.VMEM((width, width), BF16),
        ]
        + work(tile)
        + [pltpu.SemaphoreType.DMA((4 + WIDTHS,))],
        compiler_params=params(18),
        cost_estimate=cost,
        name="attend_own",
    )(which, *(pltpu.with_memory_space_constraint(value, pltpu.HBM) for value in (atoms, edge_mask)), gain,
      *(pltpu.with_memory_space_constraint(value, pltpu.HBM) for value in (w_query, w_key, w_value)))
    for rows, slot in ((mate, 1), (across, 2), (passed, 3), (far0, 4)):
        sums = pl.pallas_call(
            functools.partial(next_kernel, slot=slot),
            in_specs=[vmem] * 7,
            out_specs=vmem,
            out_shape=state,
            scratch_shapes=work(rows.shape[0]),
            compiler_params=params(12),
            cost_estimate=cost,
        )(rows, gain, w_key, w_value, query_heads, bias, sums)
    after, stats = pl.pallas_call(
        functools.partial(last_kernel, slot=WIDTHS - 1, first=half),
        in_specs=[vmem] * 9,
        out_specs=[vmem] * 2,
        out_shape=[
            jax.ShapeDtypeStruct((tile, width), F32),
            jax.ShapeDtypeStruct((2, width), F32),
        ],
        scratch_shapes=work(half) + [pltpu.VMEM(state.shape, F32)],
        compiler_params=params(12),
        cost_estimate=cost,
        name="attend_far1",
    )(far1, gain, w_key, w_value, query_heads, bias, sums, atoms, w_out)
    mean, var = merged(stats, tile, "blk")
    batched = ((after - mean) * lax.rsqrt(var + 1e-05) * bn_gain + bn_shift).astype(BF16)
    hidden = jax.nn.gelu(
        jnp.dot(batched, w_up, preferred_element_type=F32), approximate=True
    ).astype(BF16)
    return (after + jnp.dot(hidden, w_down, preferred_element_type=F32)).astype(BF16)


def solution(mesh):
    rows = P(("grp", "blk"), None)
    placed = (rows, P(("grp", "blk"), None, None, None)) + (P(),) * 9


    return jax.shard_map(body, mesh=mesh, in_specs=placed, out_specs=rows, check_vma=False)
```

```python
import functools

import jax
import jax.numpy as jnp
from jax import lax
from jax.experimental import pallas as pl
from jax.experimental.pallas import tpu as pltpu
from jax.sharding import PartitionSpec as P


HEADS = 8
HEAD_DIM = 64
REACH = 2
WIDTHS = 2 * REACH + 1
PAIR = 2 * HEAD_DIM
ROWS = 8
TOTAL = HEAD_DIM
SHIFT = HEAD_DIM + ROWS
DEPTH = HEAD_DIM + 2 * ROWS
BLOCKED = -1e30
LOG2E = 1.4426950408889634
LIMIT = 2.0**80
F32 = jnp.float32
BF16 = jnp.bfloat16


def moved(value, axis, target):
    count = lax.axis_size(axis)
    pairs = [(source, target(source) % count) for source in range(count)]
    return lax.ppermute(value, axis, pairs)


def normalised(rows, gain):
    rows = rows.astype(F32)
    scale = lax.rsqrt(jnp.mean(rows * rows, axis=-1, keepdims=True) + 1e-06)
    return (rows * scale * gain).astype(BF16)


def fill_keys(normed, w_key, keys_ref):
    keys = jnp.dot(normed, w_key, preferred_element_type=F32).astype(BF16)
    for pair in range(HEADS // 2):
        keys_ref[pair] = keys[:, pair * PAIR : (pair + 1) * PAIR]


def fill_values(normed, w_value, values_ref):
    values = jnp.dot(normed, w_value, preferred_element_type=F32).astype(BF16)
    values_t = jnp.transpose(values)
    row = lax.broadcasted_iota(jnp.int32, (2 * ROWS, values_t.shape[1]), 0)
    ones = jnp.where(row < ROWS, 1.0, 0.0).astype(BF16)
    for head in range(HEADS):
        values_ref[head, :HEAD_DIM, :] = values_t[head * HEAD_DIM : (head + 1) * HEAD_DIM]
        values_ref[head, HEAD_DIM:, :] = ones


def bias_of(mask, own):
    tile = mask.shape[0]
    allowed = mask > 0
    if own:
        rows = lax.broadcasted_iota(jnp.int32, (tile, tile), 0)
        cols = lax.broadcasted_iota(jnp.int32, (tile, tile), 1)
        allowed = allowed | (rows == cols)
    bias = jnp.where(allowed, 0.0, BLOCKED).astype(BF16)
    return jnp.transpose(bias).astype(F32)


def attend(rows, gain, w_key, w_value, query_ref, bias_ref, keep, work, old, new):
    keys_ref, values_ref = work
    slot, first = keep
    count, tile = rows.shape[0], bias_ref.shape[-1]
    ahead = 1 if 2 * count > tile else 2
    normed = normalised(rows, gain)
    fill_keys(normed, w_key, keys_ref)

    def raw(head):
        return jnp.dot(keys_ref[head // 2], query_ref[head], preferred_element_type=F32)

    def scores(product):
        return product * LOG2E + bias_ref[slot, first : first + count]

    def mix(head, weight):
        return jnp.dot(values_ref[head], weight.astype(BF16), preferred_element_type=F32)

    pending = [raw(head) for head in range(ahead)]
    fill_values(normed, w_value, values_ref)
    strayed = jnp.zeros((ROWS, tile), F32)
    for head in range(HEADS):
        if head + ahead < HEADS:
            pending.append(raw(head + ahead))
        mixed = mix(head, jnp.exp2(scores(pending.pop(0))))
        if old is not None:
            mixed = old[head] + mixed
        new[head] = mixed
        total, shift = mixed[TOTAL:SHIFT], mixed[SHIFT:]
        fits = (total <= LIMIT) & (total >= 1.0 / LIMIT) & (shift == 0.0)
        strayed = jnp.where(fits, strayed, 1.0)

    @pl.when(jnp.max(strayed) > 0.0)
    def _():
        def one_head(head, carry):
            score = scores(raw(head))
            top = jnp.max(score, axis=0, keepdims=True)
            if old is not None:
                before = old[head, SHIFT : SHIFT + 1]
                top = jnp.maximum(before, top)
            mixed = mix(head, jnp.exp2(score - top))
            if old is not None:
                mixed = old[head] * jnp.exp2(before - top) + mixed
            new[head] = mixed
            new[head, SHIFT:] = jnp.broadcast_to(top, (ROWS, tile))
            return carry

        lax.fori_loop(0, HEADS, one_head, 0)


def first_kernel(
    which_ref, own_hbm, mask_hbm, gain_hbm, w_query_hbm, w_key_hbm, w_value_hbm,
    query_ref, bias_ref, sum_ref, piece_ref,
    own_ref, mask_ref, gain_ref, w_query_ref, w_key_ref, w_value_ref,
    keys_ref, values_ref, sems,
):
    fetches = [
        pltpu.make_async_copy(source, target, sems.at[index])
        for index, (source, target) in enumerate(
            [
                (own_hbm, own_ref),
                (gain_hbm, gain_ref),
                (w_query_hbm, w_query_ref),
                (w_key_hbm, w_key_ref),
                (w_value_hbm, w_value_ref),
            ]
            + [(mask_hbm.at[0, offset], mask_ref.at[offset]) for offset in range(WIDTHS)]
        )
    ]
    for fetch in fetches:
        fetch.start()
    fetches[0].wait()
    piece_ref[...] = own_ref[: piece_ref.shape[0], :]
    fetches[1].wait()
    normed = normalised(own_ref[...], gain_ref[...])
    fetches[2].wait()
    query = jnp.dot(normed, w_query_ref[...], preferred_element_type=F32).astype(BF16)
    query_t = jnp.transpose(query * jnp.asarray(HEAD_DIM ** (-0.5), BF16))
    tile = query_t.shape[1]
    for head in range(HEADS):
        half = (head % 2) * HEAD_DIM
        query_ref[head, half : half + HEAD_DIM, :] = query_t[
            head * HEAD_DIM : (head + 1) * HEAD_DIM
        ]
        query_ref[head, HEAD_DIM - half : PAIR - half, :] = jnp.zeros((HEAD_DIM, tile), BF16)
    for fetch in fetches[3:]:
        fetch.wait()
    for slot in range(WIDTHS):
        bias_ref[slot] = bias_of(mask_ref[which_ref[slot]], slot == 0)
    attend(
        own_ref[...], gain_ref[...], w_key_ref[...], w_value_ref[...], query_ref, bias_ref,
        (0, 0), (keys_ref, values_ref), None, sum_ref,
    )


def next_kernel(
    rows_ref, gain_ref, w_key_ref, w_value_ref, query_ref, bias_ref, sum_in,
    sum_ref, keys_ref, values_ref, *, slot, first=0,
):
    attend(
        rows_ref[...], gain_ref[...], w_key_ref[...], w_value_ref[...], query_ref, bias_ref,
        (slot, first), (keys_ref, values_ref), sum_in, sum_ref,
    )


def last_kernel(
    rows_ref, gain_ref, w_key_ref, w_value_ref, query_ref, bias_ref, sum_in,
    own_ref, w_out_ref, after_ref, stats_ref,
    keys_ref, values_ref, sum_ref, *, slot, first,
):
    next_kernel(
        rows_ref, gain_ref, w_key_ref, w_value_ref, query_ref, bias_ref, sum_in,
        sum_ref, keys_ref, values_ref, slot=slot, first=first,
    )
    mixed_t = jnp.concatenate(
        [
            (sum_ref[head, :HEAD_DIM] * (1.0 / sum_ref[head, TOTAL : TOTAL + 1])).astype(BF16)
            for head in range(HEADS)
        ],
        axis=0,
    )
    mixed = jnp.transpose(mixed_t)
    after = own_ref[...].astype(F32) + jnp.dot(
        mixed, w_out_ref[...], preferred_element_type=F32
    )
    after_ref[...] = after
    mean = jnp.mean(after, axis=0, keepdims=True)
    centered = after - mean
    stats_ref[0:1, :] = mean
    stats_ref[1:2, :] = jnp.sum(centered * centered, axis=0, keepdims=True)


def pick_kernel(flag_ref, yes_ref, no_ref, out_ref):
    first = yes_ref.shape[0] - out_ref.shape[0]
    for value, source in ((1, yes_ref), (0, no_ref)):

        @pl.when(flag_ref[WIDTHS] == value)
        def _():
            out_ref[...] = source[first:, :]


def joined(parts, rows):
    mean = sum(part[0] for part in parts) * (1.0 / len(parts))
    spread = sum(part[1] + rows * jnp.square(part[0] - mean) for part in parts)
    return jnp.stack([mean, spread])


def merged(stats, rows, axis):
    count = lax.axis_size(axis)
    step = 1
    while step < count:
        if count % (16 * step) == 0 and step == 1:
            stats = joined([stats, moved(stats, axis, lambda s: s ^ 1)], rows)
            side = lax.axis_index(axis) % 2
            last = moved(stats, axis, lambda s: s ^ 8)
            found = [
                moved(stats, axis, lambda s, peer=peer: s ^ (8 * (s % 2) + 2 * peer))
                for peer in (1, 2, 3)
            ]
            stats = joined([jnp.where(side == 0, stats, last)] + found, 2 * rows)
            stats = joined([stats, moved(stats, axis, lambda s: s ^ 1)], 8 * rows)
            step, rows = 16, 16 * rows
        else:
            stats = joined([stats, moved(stats, axis, lambda s: s ^ step)], rows)
            step, rows = 2 * step, 2 * rows
    return stats[0], stats[1] / rows


def body(
    atoms, edge_mask, norm_gain, w_query, w_key, w_value, w_out, bn_gain, bn_shift, w_up, w_down
):
    tile, width = atoms.shape
    place = lax.axis_index("blk") % 4
    sign = 1 - 2 * (place % 2)
    inner = (place + 1) // 2 % 2
    which = jnp.stack(
        [REACH + 0 * sign, REACH + sign, REACH - sign, REACH + 2 * sign, REACH - 2 * sign, inner]
    )
    across = moved(atoms, "blk", lambda s: s + 1 if s % 2 else s - 1)
    mate = moved(atoms, "blk", lambda s: s ^ 1)
    gain = norm_gain.reshape(1, width)

    vmem = pl.BlockSpec(memory_space=pltpu.VMEM)
    hbm = pl.BlockSpec(memory_space=pltpu.HBM)
    smem = pl.BlockSpec(memory_space=pltpu.SMEM)
    state = jax.ShapeDtypeStruct((HEADS, DEPTH, tile), F32)

    def work(rows):
        return [
            pltpu.VMEM((HEADS // 2, rows, PAIR), BF16),
            pltpu.VMEM((HEADS, DEPTH, rows), BF16),
        ]


    def params(mib):
        return pltpu.CompilerParams(vmem_limit_bytes=mib * 1024 * 1024)

    cost = pl.CostEstimate(
        flops=8 * tile * tile * width, bytes_accessed=4 * tile * width, transcendentals=0
    )

    passed = moved(across, "blk", lambda s: s ^ 1)
    half = tile // 2
    forward = pl.pallas_call(
        pick_kernel,
        in_specs=[smem, vmem, vmem],
        out_specs=vmem,
        out_shape=jax.ShapeDtypeStruct((half, width), BF16),
        compiler_params=params(2),
        name="pick_far",
    )(which, across, atoms)
    far1 = moved(forward, "blk", lambda s: s + (2, 3, -3, -2)[s % 4])

    query_heads, bias, sums, piece = pl.pallas_call(
        first_kernel,
        in_specs=[smem] + [hbm] * 6,
        out_specs=[vmem] * 4,
        out_shape=[
            jax.ShapeDtypeStruct((HEADS, PAIR, tile), BF16),
            jax.ShapeDtypeStruct((WIDTHS, tile, tile), F32),
            state,
            jax.ShapeDtypeStruct((half, width), BF16),
        ],
        scratch_shapes=[
            pltpu.VMEM((tile, width), BF16),
            pltpu.VMEM((WIDTHS, tile, tile), jnp.int32),
            pltpu.VMEM((1, width), F32),
            pltpu.VMEM((width, width), BF16),
            pltpu.VMEM((width, width), BF16),
            pltpu.VMEM((width, width), BF16),
        ]
        + work(tile)
        + [pltpu.SemaphoreType.DMA((5 + WIDTHS,))],
        compiler_params=params(18),
        cost_estimate=cost,
        name="attend_own",
    )(
        which,
        *(
            pltpu.with_memory_space_constraint(value, pltpu.HBM)
            for value in (atoms, edge_mask, gain, w_query, w_key, w_value)
        ),
    )
    far0 = moved(piece, "blk", lambda s: s - 2 if s % 2 else s + 2)
    for rows, slot in ((mate, 1), (across, 2), (passed, 3), (far0, 4)):
        sums = pl.pallas_call(
            functools.partial(next_kernel, slot=slot),
            in_specs=[vmem] * 7,
            out_specs=vmem,
            out_shape=state,
            scratch_shapes=work(rows.shape[0]),
            compiler_params=params(12),
            cost_estimate=cost,
        )(rows, gain, w_key, w_value, query_heads, bias, sums)
    after, stats = pl.pallas_call(
        functools.partial(last_kernel, slot=WIDTHS - 1, first=half),
        in_specs=[vmem] * 9,
        out_specs=[vmem] * 2,
        out_shape=[
            jax.ShapeDtypeStruct((tile, width), F32),
            jax.ShapeDtypeStruct((2, width), F32),
        ],
        scratch_shapes=work(half) + [pltpu.VMEM(state.shape, F32)],
        compiler_params=params(12),
        cost_estimate=cost,
        name="attend_far1",
    )(far1, gain, w_key, w_value, query_heads, bias, sums, atoms, w_out)
    mean, var = merged(stats, tile, "blk")
    batched = ((after - mean) * lax.rsqrt(var + 1e-05) * bn_gain + bn_shift).astype(BF16)
    hidden = jax.nn.gelu(
        jnp.dot(batched, w_up, preferred_element_type=F32), approximate=True
    ).astype(BF16)
    return (after + jnp.dot(hidden, w_down, preferred_element_type=F32)).astype(BF16)


def solution(mesh):
    rows = P(("grp", "blk"), None)
    placed = (rows, P(("grp", "blk"), None, None, None)) + (P(),) * 9


    return jax.shard_map(body, mesh=mesh, in_specs=placed, out_specs=rows, check_vma=False)
```

```python
import functools

import jax
import jax.numpy as jnp
from jax import lax
from jax.experimental import pallas as pl
from jax.experimental.pallas import tpu as pltpu
from jax.sharding import PartitionSpec as P


HEADS = 8
HEAD_DIM = 64
REACH = 2
WIDTHS = 2 * REACH + 1
PAIR = 2 * HEAD_DIM
ROWS = 8
TOTAL = HEAD_DIM
SHIFT = HEAD_DIM + ROWS
DEPTH = HEAD_DIM + 2 * ROWS
BLOCKED = -1e30
LOG2E = 1.4426950408889634
LIMIT = 2.0**80
F32 = jnp.float32
BF16 = jnp.bfloat16


def moved(value, axis, target):
    count = lax.axis_size(axis)
    pairs = [(source, target(source) % count) for source in range(count)]
    return lax.ppermute(value, axis, pairs)


def normalised(rows, gain):
    rows = rows.astype(F32)
    scale = lax.rsqrt(jnp.mean(rows * rows, axis=-1, keepdims=True) + 1e-06)
    return (rows * scale * gain).astype(BF16)


def fill_keys(normed, w_key, keys_ref):
    keys = jnp.dot(normed, w_key, preferred_element_type=F32).astype(BF16)
    for pair in range(HEADS // 2):
        keys_ref[pair] = keys[:, pair * PAIR : (pair + 1) * PAIR]


def fill_values(normed, w_value, values_ref):
    values = jnp.dot(normed, w_value, preferred_element_type=F32).astype(BF16)
    values_t = jnp.transpose(values)
    row = lax.broadcasted_iota(jnp.int32, (2 * ROWS, values_t.shape[1]), 0)
    ones = jnp.where(row < ROWS, 1.0, 0.0).astype(BF16)
    for head in range(HEADS):
        values_ref[head, :HEAD_DIM, :] = values_t[head * HEAD_DIM : (head + 1) * HEAD_DIM]
        values_ref[head, HEAD_DIM:, :] = ones


def bias_of(mask, own):
    tile = mask.shape[0]
    allowed = mask > 0
    if own:
        rows = lax.broadcasted_iota(jnp.int32, (tile, tile), 0)
        cols = lax.broadcasted_iota(jnp.int32, (tile, tile), 1)
        allowed = allowed | (rows == cols)
    bias = jnp.where(allowed, 0.0, BLOCKED).astype(BF16)
    return jnp.transpose(bias).astype(F32)


def attend(rows, gain, w_key, w_value, query_ref, bias_ref, keep, work, old, new, finish=None):
    keys_ref, values_ref = work
    slot, first = keep
    count, tile = rows.shape[0], bias_ref.shape[-1]
    ahead = 1 if 2 * count > tile else 2
    normed = normalised(rows, gain)
    fill_keys(normed, w_key, keys_ref)

    def raw(head):
        return jnp.dot(keys_ref[head // 2], query_ref[head], preferred_element_type=F32)

    def scores(product):
        return product * LOG2E + bias_ref[slot, first : first + count]

    def mix(head, weight):
        return jnp.dot(values_ref[head], weight.astype(BF16), preferred_element_type=F32)

    fill_values(normed, w_value, values_ref)
    pending = [raw(head) for head in range(ahead)]
    strayed = jnp.zeros((ROWS, tile), F32)
    for head in range(HEADS):
        if head + ahead < HEADS:
            pending.append(raw(head + ahead))
        mixed = mix(head, jnp.exp2(scores(pending.pop(0))))
        if old is not None:
            mixed = old[head] + mixed
        new[head] = mixed
        total, shift = mixed[TOTAL:SHIFT], mixed[SHIFT:]
        fits = (total <= LIMIT) & (total >= 1.0 / LIMIT) & (shift == 0.0)
        strayed = jnp.where(fits, strayed, 1.0)

    if finish is not None:
        finish()

    @pl.when(jnp.max(strayed) > 0.0)
    def _():
        def one_head(head, carry):
            score = scores(raw(head))
            top = jnp.max(score, axis=0, keepdims=True)
            if old is not None:
                before = old[head, SHIFT : SHIFT + 1]
                top = jnp.maximum(before, top)
            mixed = mix(head, jnp.exp2(score - top))
            if old is not None:
                mixed = old[head] * jnp.exp2(before - top) + mixed
            new[head] = mixed
            new[head, SHIFT:] = jnp.broadcast_to(top, (ROWS, tile))
            return carry

        lax.fori_loop(0, HEADS, one_head, 0)
        if finish is not None:
            finish()


def first_kernel(
    which_ref, own_hbm, mask_hbm, gain_hbm, w_query_hbm, w_key_hbm, w_value_hbm,
    query_ref, bias_ref, sum_ref, piece_ref, flag_ref,
    own_ref, mask_ref, gain_ref, w_query_ref, w_key_ref, w_value_ref,
    keys_ref, values_ref, sems,
):
    fetches = [
        pltpu.make_async_copy(source, target, sems.at[index])
        for index, (source, target) in enumerate(
            [
                (own_hbm, own_ref),
                (gain_hbm, gain_ref),
                (w_query_hbm, w_query_ref),
                (w_key_hbm, w_key_ref),
                (w_value_hbm, w_value_ref),
            ]
            + [(mask_hbm.at[0, offset], mask_ref.at[offset]) for offset in range(WIDTHS)]
        )
    ]
    for fetch in fetches:
        fetch.start()
    flag_ref[...] = jnp.full(flag_ref.shape, which_ref[WIDTHS], jnp.int32)
    fetches[0].wait()
    piece_ref[...] = own_ref[: piece_ref.shape[0], :]
    fetches[1].wait()
    normed = normalised(own_ref[...], gain_ref[...])
    fetches[2].wait()
    query = jnp.dot(normed, w_query_ref[...], preferred_element_type=F32).astype(BF16)
    query_t = jnp.transpose(query * jnp.asarray(HEAD_DIM ** (-0.5), BF16))
    tile = query_t.shape[1]
    for head in range(HEADS):
        half = (head % 2) * HEAD_DIM
        query_ref[head, half : half + HEAD_DIM, :] = query_t[
            head * HEAD_DIM : (head + 1) * HEAD_DIM
        ]
        query_ref[head, HEAD_DIM - half : PAIR - half, :] = jnp.zeros((HEAD_DIM, tile), BF16)
    for fetch in fetches[3:]:
        fetch.wait()
    for slot in range(WIDTHS):
        bias_ref[slot] = bias_of(mask_ref[which_ref[slot]], slot == 0)
    attend(
        own_ref[...], gain_ref[...], w_key_ref[...], w_value_ref[...], query_ref, bias_ref,
        (0, 0), (keys_ref, values_ref), None, sum_ref,
    )


def next_kernel(
    rows_ref, gain_ref, w_key_ref, w_value_ref, query_ref, bias_ref, sum_in,
    sum_ref, keys_ref, values_ref, *, slot, first=0,
):
    attend(
        rows_ref[...], gain_ref[...], w_key_ref[...], w_value_ref[...], query_ref, bias_ref,
        (slot, first), (keys_ref, values_ref), sum_in, sum_ref,
    )


def last_kernel(
    rows_ref, gain_ref, w_key_ref, w_value_ref, query_ref, bias_ref, sum_in,
    own_ref, w_out_ref, after_ref, stats_ref,
    keys_ref, values_ref, sum_ref, *, slot, first,
):
    def finish():
        mixed_t = jnp.concatenate(
            [
                (sum_ref[head, :HEAD_DIM] * (1.0 / sum_ref[head, TOTAL : TOTAL + 1])).astype(BF16)
                for head in range(HEADS)
            ],
            axis=0,
        )
        mixed = jnp.transpose(mixed_t)
        after = own_ref[...].astype(F32) + jnp.dot(
            mixed, w_out_ref[...], preferred_element_type=F32
        )
        after_ref[...] = after
        mean = jnp.mean(after, axis=0, keepdims=True)
        centered = after - mean
        stats_ref[0:1, :] = mean
        stats_ref[1:2, :] = jnp.sum(centered * centered, axis=0, keepdims=True)

    attend(
        rows_ref[...], gain_ref[...], w_key_ref[...], w_value_ref[...], query_ref, bias_ref,
        (slot, first), (keys_ref, values_ref), sum_in, sum_ref, finish,
    )


def pick_kernel(flag_ref, yes_ref, no_ref, out_ref):
    first = yes_ref.shape[0] - out_ref.shape[0]
    out_ref[...] = jnp.where(
        flag_ref[...] > 0, yes_ref[first:, :].astype(F32), no_ref[first:, :].astype(F32)
    ).astype(BF16)


def joined(parts, rows):
    mean = sum(part[0] for part in parts) * (1.0 / len(parts))
    spread = sum(part[1] + rows * jnp.square(part[0] - mean) for part in parts)
    return jnp.stack([mean, spread])


def merged(stats, rows, axis):
    count = lax.axis_size(axis)
    if count & (count - 1):
        every = lax.all_gather(stats, axis)
        stats = joined([every[place] for place in range(count)], rows)
        return stats[0], stats[1] / (count * rows)
    step = 1
    while step < count:
        if count % (16 * step) == 0 and step == 1:
            stats = joined([stats, moved(stats, axis, lambda s: s ^ 1)], rows)
            side = lax.axis_index(axis) % 2
            last = moved(stats, axis, lambda s: s ^ 8)
            found = [
                moved(stats, axis, lambda s, peer=peer: s ^ (8 * (s % 2) + 2 * peer))
                for peer in (1, 2, 3)
            ]
            stats = joined([jnp.where(side == 0, stats, last)] + found, 2 * rows)
            stats = joined([stats, moved(stats, axis, lambda s: s ^ 1)], 8 * rows)
            step, rows = 16, 16 * rows
        else:
            stats = joined([stats, moved(stats, axis, lambda s: s ^ step)], rows)
            step, rows = 2 * step, 2 * rows
    return stats[0], stats[1] / rows


def body(
    atoms, edge_mask, norm_gain, w_query, w_key, w_value, w_out, bn_gain, bn_shift, w_up, w_down
):
    tile, width = atoms.shape
    place = lax.axis_index("blk") % 4
    sign = 1 - 2 * (place % 2)
    which = jnp.stack(
        [REACH + 0 * sign, REACH + sign, REACH - sign, REACH + 2 * sign, REACH - 2 * sign]
        + [(place + 1) // 2 % 2]
    )
    across = moved(atoms, "blk", lambda s: s + 1 if s % 2 else s - 1)
    mate = moved(atoms, "blk", lambda s: s ^ 1)
    gain = norm_gain.reshape(1, width)

    vmem = pl.BlockSpec(memory_space=pltpu.VMEM)
    hbm = pl.BlockSpec(memory_space=pltpu.HBM)
    smem = pl.BlockSpec(memory_space=pltpu.SMEM)
    state = jax.ShapeDtypeStruct((HEADS, DEPTH, tile), F32)

    def work(rows):
        return [
            pltpu.VMEM((HEADS // 2, rows, PAIR), BF16),
            pltpu.VMEM((HEADS, DEPTH, rows), BF16),
        ]

    def params(mib):
        return pltpu.CompilerParams(vmem_limit_bytes=mib * 1024 * 1024)

    cost = pl.CostEstimate(
        flops=8 * tile * tile * width, bytes_accessed=4 * tile * width, transcendentals=0
    )

    passed = moved(across, "blk", lambda s: s ^ 1)
    half = tile // 2
    query_heads, bias, sums, piece, inner = pl.pallas_call(
        first_kernel,
        in_specs=[smem] + [hbm] * 6,
        out_specs=[vmem] * 5,
        out_shape=[
            jax.ShapeDtypeStruct((HEADS, PAIR, tile), BF16),
            jax.ShapeDtypeStruct((WIDTHS, tile, tile), F32),
            state,
            jax.ShapeDtypeStruct((half, width), BF16),
            jax.ShapeDtypeStruct((1, width), jnp.int32),
        ],
        scratch_shapes=[
            pltpu.VMEM((tile, width), BF16),
            pltpu.VMEM((WIDTHS, tile, tile), jnp.int32),
            pltpu.VMEM((1, width), F32),
            pltpu.VMEM((width, width), BF16),
            pltpu.VMEM((width, width), BF16),
            pltpu.VMEM((width, width), BF16),
        ]
        + work(tile)
        + [pltpu.SemaphoreType.DMA((5 + WIDTHS,))],
        compiler_params=params(18),
        cost_estimate=cost,
        name="attend_own",
    )(
        which,
        *(
            pltpu.with_memory_space_constraint(value, pltpu.HBM)
            for value in (atoms, edge_mask, gain, w_query, w_key, w_value)
        ),
    )
    far0 = moved(piece, "blk", lambda s: s - 2 if s % 2 else s + 2)
    forward = pl.pallas_call(
        pick_kernel,
        in_specs=[vmem] * 3,
        out_specs=vmem,
        out_shape=jax.ShapeDtypeStruct((half, width), BF16),
        compiler_params=params(2),
        name="pick_far",
    )(inner, across, atoms)
    far1 = moved(forward, "blk", lambda s: s + (2, 3, -3, -2)[s % 4])
    for rows, slot in ((mate, 1), (across, 2), (passed, 3), (far0, 4)):
        sums = pl.pallas_call(
            functools.partial(next_kernel, slot=slot),
            in_specs=[vmem] * 7,
            out_specs=vmem,
            out_shape=state,
            scratch_shapes=work(rows.shape[0]),
            compiler_params=params(12),
            cost_estimate=cost,
        )(rows, gain, w_key, w_value, query_heads, bias, sums)
    after, stats = pl.pallas_call(
        functools.partial(last_kernel, slot=WIDTHS - 1, first=half),
        in_specs=[vmem] * 9,
        out_specs=[vmem] * 2,
        out_shape=[
            jax.ShapeDtypeStruct((tile, width), F32),
            jax.ShapeDtypeStruct((2, width), F32),
        ],
        scratch_shapes=work(half) + [pltpu.VMEM(state.shape, F32)],
        compiler_params=params(12),
        cost_estimate=cost,
        name="attend_far1",
    )(far1, gain, w_key, w_value, query_heads, bias, sums, atoms, w_out)
    mean, var = merged(stats, tile, "blk")
    batched = ((after - mean) * lax.rsqrt(var + 1e-05) * bn_gain + bn_shift).astype(BF16)
    hidden = jax.nn.gelu(
        jnp.dot(batched, w_up, preferred_element_type=F32), approximate=True
    ).astype(BF16)
    return (after + jnp.dot(hidden, w_down, preferred_element_type=F32)).astype(BF16)


def solution(mesh):
    rows = P(("grp", "blk"), None)
    placed = (rows, P(("grp", "blk"), None, None, None)) + (P(),) * 9


    return jax.shard_map(body, mesh=mesh, in_specs=placed, out_specs=rows, check_vma=False)
```

```python
import functools

import jax
import jax.numpy as jnp
from jax import lax
from jax.experimental import pallas as pl
from jax.experimental.pallas import tpu as pltpu
from jax.sharding import PartitionSpec as P


HEADS = 8
HEAD_DIM = 64
REACH = 2
WIDTHS = 2 * REACH + 1
PAIR = 2 * HEAD_DIM
ROWS = 8
TOTAL = HEAD_DIM
SHIFT = HEAD_DIM + ROWS
DEPTH = HEAD_DIM + 2 * ROWS
BLOCKED = -1e30
LOG2E = 1.4426950408889634
LIMIT = 2.0**80
GELU = 0.7978845608028654
F32 = jnp.float32
BF16 = jnp.bfloat16


def moved(value, axis, target):
    count = lax.axis_size(axis)
    pairs = [(source, target(source) % count) for source in range(count)]
    return lax.ppermute(value, axis, pairs)


def normalised(rows, gain):
    rows = rows.astype(F32)
    scale = lax.rsqrt(jnp.mean(rows * rows, axis=-1, keepdims=True) + 1e-06)
    return (rows * scale * gain).astype(BF16)


def fill_keys(normed, w_key, keys_ref):
    keys = jnp.dot(normed, w_key, preferred_element_type=F32).astype(BF16)
    for pair in range(HEADS // 2):
        keys_ref[pair] = keys[:, pair * PAIR : (pair + 1) * PAIR]


def fill_values(normed, w_value, values_ref):
    values = jnp.dot(normed, w_value, preferred_element_type=F32).astype(BF16)
    values_t = jnp.transpose(values)
    row = lax.broadcasted_iota(jnp.int32, (2 * ROWS, values_t.shape[1]), 0)
    ones = jnp.where(row < ROWS, 1.0, 0.0).astype(BF16)
    for head in range(HEADS):
        values_ref[head, :HEAD_DIM, :] = values_t[head * HEAD_DIM : (head + 1) * HEAD_DIM]
        values_ref[head, HEAD_DIM:, :] = ones


def bias_of(mask, own):
    tile = mask.shape[0]
    allowed = mask > 0
    if own:
        rows = lax.broadcasted_iota(jnp.int32, (tile, tile), 0)
        cols = lax.broadcasted_iota(jnp.int32, (tile, tile), 1)
        allowed = allowed | (rows == cols)
    bias = jnp.where(allowed, 0.0, BLOCKED).astype(BF16)
    return jnp.transpose(bias).astype(F32)


def attend(rows, gain, w_key, w_value, query_ref, bias_ref, keep, work, old, new, finish=None):
    keys_ref, values_ref = work
    slot, first = keep
    count, tile = rows.shape[0], bias_ref.shape[-1]
    ahead = 1 if 2 * count > tile else 2
    normed = normalised(rows, gain)
    fill_keys(normed, w_key, keys_ref)

    def raw(head):
        return jnp.dot(keys_ref[head // 2], query_ref[head], preferred_element_type=F32)

    def scores(product):
        return product * LOG2E + bias_ref[slot, first : first + count]

    def mix(head, weight):
        return jnp.dot(values_ref[head], weight.astype(BF16), preferred_element_type=F32)

    fill_values(normed, w_value, values_ref)
    pending = [raw(head) for head in range(ahead)]
    strayed = jnp.zeros((ROWS, tile), F32)
    for head in range(HEADS):
        if head + ahead < HEADS:
            pending.append(raw(head + ahead))
        mixed = mix(head, jnp.exp2(scores(pending.pop(0))))
        if old is not None:
            mixed = old[head] + mixed
        new[head] = mixed
        total, shift = mixed[TOTAL:SHIFT], mixed[SHIFT:]
        fits = (total <= LIMIT) & (total >= 1.0 / LIMIT) & (shift == 0.0)
        strayed = jnp.where(fits, strayed, 1.0)

    if finish is not None:
        finish()

    @pl.when(jnp.max(strayed) > 0.0)
    def _():
        def one_head(head, carry):
            score = scores(raw(head))
            top = jnp.max(score, axis=0, keepdims=True)
            if old is not None:
                before = old[head, SHIFT : SHIFT + 1]
                top = jnp.maximum(before, top)
            mixed = mix(head, jnp.exp2(score - top))
            if old is not None:
                mixed = old[head] * jnp.exp2(before - top) + mixed
            new[head] = mixed
            new[head, SHIFT:] = jnp.broadcast_to(top, (ROWS, tile))
            return carry

        lax.fori_loop(0, HEADS, one_head, 0)
        if finish is not None:
            finish()


def first_kernel(
    which_ref, own_hbm, mask_hbm, gain_hbm, w_query_hbm, w_key_hbm, w_value_hbm,
    query_ref, bias_ref, sum_ref, piece_ref, flag_ref,
    own_ref, mask_ref, gain_ref, w_query_ref, w_key_ref, w_value_ref,
    keys_ref, values_ref, sems,
):
    fetches = [
        pltpu.make_async_copy(source, target, sems.at[index])
        for index, (source, target) in enumerate(
            [
                (own_hbm, own_ref),
                (gain_hbm, gain_ref),
                (w_query_hbm, w_query_ref),
                (w_key_hbm, w_key_ref),
                (w_value_hbm, w_value_ref),
            ]
            + [(mask_hbm.at[0, offset], mask_ref.at[offset]) for offset in range(WIDTHS)]
        )
    ]
    for fetch in fetches:
        fetch.start()
    flag_ref[...] = jnp.full(flag_ref.shape, which_ref[WIDTHS], jnp.int32)
    fetches[0].wait()
    piece_ref[...] = own_ref[: piece_ref.shape[0], :]
    fetches[1].wait()
    normed = normalised(own_ref[...], gain_ref[...])
    fetches[2].wait()
    query = jnp.dot(normed, w_query_ref[...], preferred_element_type=F32).astype(BF16)
    query_t = jnp.transpose(query * jnp.asarray(HEAD_DIM ** (-0.5), BF16))
    tile = query_t.shape[1]
    for head in range(HEADS):
        half = (head % 2) * HEAD_DIM
        query_ref[head, half : half + HEAD_DIM, :] = query_t[
            head * HEAD_DIM : (head + 1) * HEAD_DIM
        ]
        query_ref[head, HEAD_DIM - half : PAIR - half, :] = jnp.zeros((HEAD_DIM, tile), BF16)
    for fetch in fetches[3:]:
        fetch.wait()
    for slot in range(WIDTHS):
        bias_ref[slot] = bias_of(mask_ref[which_ref[slot]], slot == 0)
    attend(
        own_ref[...], gain_ref[...], w_key_ref[...], w_value_ref[...], query_ref, bias_ref,
        (0, 0), (keys_ref, values_ref), None, sum_ref,
    )


def next_kernel(
    rows_ref, gain_ref, w_key_ref, w_value_ref, query_ref, bias_ref, sum_in,
    sum_ref, keys_ref, values_ref, *, slot, first=0,
):
    attend(
        rows_ref[...], gain_ref[...], w_key_ref[...], w_value_ref[...], query_ref, bias_ref,
        (slot, first), (keys_ref, values_ref), sum_in, sum_ref,
    )


def last_kernel(
    rows_ref, gain_ref, w_key_ref, w_value_ref, query_ref, bias_ref, sum_in,
    own_ref, w_out_ref, after_ref, stats_ref,
    keys_ref, values_ref, sum_ref, *, slot, first,
):
    def finish():
        mixed_t = jnp.concatenate(
            [
                (sum_ref[head, :HEAD_DIM] * (1.0 / sum_ref[head, TOTAL : TOTAL + 1])).astype(BF16)
                for head in range(HEADS)
            ],
            axis=0,
        )
        mixed = jnp.transpose(mixed_t)
        after = own_ref[...].astype(F32) + jnp.dot(
            mixed, w_out_ref[...], preferred_element_type=F32
        )
        after_ref[...] = after
        mean = jnp.mean(after, axis=0, keepdims=True)
        centered = after - mean
        stats_ref[0:1, :] = mean
        stats_ref[1:2, :] = jnp.sum(centered * centered, axis=0, keepdims=True)

    attend(
        rows_ref[...], gain_ref[...], w_key_ref[...], w_value_ref[...], query_ref, bias_ref,
        (slot, first), (keys_ref, values_ref), sum_in, sum_ref, finish,
    )


def forward_kernel(
    after_ref, mine_ref, other_ref, gain_ref, shift_ref, w_up_ref, w_down_ref, out_hbm, out_ref, sems,
    *, count,
):
    rows = out_ref.shape[0] // sems.shape[0]
    mean = 0.5 * (mine_ref[0:1, :] + other_ref[0:1, :])
    gap = mine_ref[0:1, :] - other_ref[0:1, :]
    var = (mine_ref[1:2, :] + other_ref[1:2, :]) * (1.0 / count) + 0.25 * gap * gap
    scale = lax.rsqrt(var + 1e-05) * gain_ref[...]

    def up(part):
        after = after_ref[part * rows : (part + 1) * rows, :]
        batched = ((after - mean) * scale + shift_ref[...]).astype(BF16)
        return jnp.dot(batched, w_up_ref[...], preferred_element_type=F32)

    copies = []
    raw = up(0)
    for part in range(sems.shape[0]):
        current = raw
        if part + 1 < sems.shape[0]:
            raw = up(part + 1)
        inner = current * (GELU + (GELU * 0.044715) * (current * current))
        halved = 0.5 * current
        hidden = (halved + halved * jnp.tanh(inner)).astype(BF16)
        block = pl.ds(part * rows, rows)
        updated = after_ref[block, :] + jnp.dot(
            hidden, w_down_ref[...], preferred_element_type=F32
        )
        out_ref[block, :] = updated.astype(BF16)
        copies.append(
            pltpu.make_async_copy(out_ref.at[block], out_hbm.at[block], sems.at[part])
        )
        copies[-1].start()
    for copy in copies:
        copy.wait()


def pick_kernel(flag_ref, yes_ref, no_ref, out_ref):
    first = yes_ref.shape[0] - out_ref.shape[0]
    out_ref[...] = jnp.where(
        flag_ref[...] > 0, yes_ref[first:, :].astype(F32), no_ref[first:, :].astype(F32)
    ).astype(BF16)


def joined(parts, rows):
    mean = sum(part[0] for part in parts) * (1.0 / len(parts))
    spread = sum(part[1] + rows * jnp.square(part[0] - mean) for part in parts)
    return jnp.stack([mean, spread])


def merged(stats, rows, axis):
    count = lax.axis_size(axis)
    if count & (count - 1):
        every = lax.all_gather(stats, axis)
        stats = joined([every[place] for place in range(count)], rows)
        return stats, stats, 2 * count * rows
    step = 1
    while True:
        if step == 1 and count % 16 == 0:
            stats = joined([stats, moved(stats, axis, lambda s: s ^ 1)], rows)
            side = lax.axis_index(axis) % 2
            last = moved(stats, axis, lambda s: s ^ 8)
            found = [
                moved(stats, axis, lambda s, peer=peer: s ^ (8 * (s % 2) + 2 * peer))
                for peer in (1, 2, 3)
            ]
            stats = joined([jnp.where(side == 0, stats, last)] + found, 2 * rows)
            other, step, rows = moved(stats, axis, lambda s: s ^ 1), 16, 16 * rows
        else:
            other, step, rows = moved(stats, axis, lambda s: s ^ step), 2 * step, 2 * rows
        if step >= count:
            return stats, other, rows
        stats = joined([stats, other], rows // 2)


def body(
    atoms, edge_mask, norm_gain, w_query, w_key, w_value, w_out, bn_gain, bn_shift, w_up, w_down
):
    tile, width = atoms.shape
    place = lax.axis_index("blk") % 4
    sign = 1 - 2 * (place % 2)
    which = jnp.stack(
        [REACH + 0 * sign, REACH + sign, REACH - sign, REACH + 2 * sign, REACH - 2 * sign]
        + [(place + 1) // 2 % 2]
    )
    across = moved(atoms, "blk", lambda s: s + 1 if s % 2 else s - 1)
    mate = moved(atoms, "blk", lambda s: s ^ 1)
    gain = norm_gain.reshape(1, width)

    vmem = pl.BlockSpec(memory_space=pltpu.VMEM)
    hbm = pl.BlockSpec(memory_space=pltpu.HBM)
    smem = pl.BlockSpec(memory_space=pltpu.SMEM)
    state = jax.ShapeDtypeStruct((HEADS, DEPTH, tile), F32)

    def work(rows):
        return [
            pltpu.VMEM((HEADS // 2, rows, PAIR), BF16),
            pltpu.VMEM((HEADS, DEPTH, rows), BF16),
        ]

    def params(mib):
        return pltpu.CompilerParams(vmem_limit_bytes=mib * 1024 * 1024)

    cost = pl.CostEstimate(
        flops=8 * tile * tile * width, bytes_accessed=4 * tile * width, transcendentals=0
    )

    passed = moved(across, "blk", lambda s: s ^ 1)
    half = tile // 2
    query_heads, bias, sums, piece, inner = pl.pallas_call(
        first_kernel,
        in_specs=[smem] + [hbm] * 6,
        out_specs=[vmem] * 5,
        out_shape=[
            jax.ShapeDtypeStruct((HEADS, PAIR, tile), BF16),
            jax.ShapeDtypeStruct((WIDTHS, tile, tile), F32),
            state,
            jax.ShapeDtypeStruct((half, width), BF16),
            jax.ShapeDtypeStruct((1, width), jnp.int32),
        ],
        scratch_shapes=[
            pltpu.VMEM((tile, width), BF16),
            pltpu.VMEM((WIDTHS, tile, tile), jnp.int32),
            pltpu.VMEM((1, width), F32),
            pltpu.VMEM((width, width), BF16),
            pltpu.VMEM((width, width), BF16),
            pltpu.VMEM((width, width), BF16),
        ]
        + work(tile)
        + [pltpu.SemaphoreType.DMA((5 + WIDTHS,))],
        compiler_params=params(18),
        cost_estimate=cost,
        name="attend_own",
    )(
        which,
        *(
            pltpu.with_memory_space_constraint(value, pltpu.HBM)
            for value in (atoms, edge_mask, gain, w_query, w_key, w_value)
        ),
    )
    far0 = moved(piece, "blk", lambda s: s - 2 if s % 2 else s + 2)
    forward = pl.pallas_call(
        pick_kernel,
        in_specs=[vmem] * 3,
        out_specs=vmem,
        out_shape=jax.ShapeDtypeStruct((half, width), BF16),
        compiler_params=params(2),
        name="pick_far",
    )(inner, across, atoms)
    far1 = moved(forward, "blk", lambda s: s + (2, 3, -3, -2)[s % 4])
    for rows, slot in ((mate, 1), (across, 2), (passed, 3), (far0, 4)):
        sums = pl.pallas_call(
            functools.partial(next_kernel, slot=slot),
            in_specs=[vmem] * 7,
            out_specs=vmem,
            out_shape=state,
            scratch_shapes=work(rows.shape[0]),
            compiler_params=params(12),
            cost_estimate=cost,
        )(rows, gain, w_key, w_value, query_heads, bias, sums)
    after, stats = pl.pallas_call(
        functools.partial(last_kernel, slot=WIDTHS - 1, first=half),
        in_specs=[vmem] * 9,
        out_specs=[vmem] * 2,
        out_shape=[
            jax.ShapeDtypeStruct((tile, width), F32),
            jax.ShapeDtypeStruct((2, width), F32),
        ],
        scratch_shapes=work(half) + [pltpu.VMEM(state.shape, F32)],
        compiler_params=params(12),
        cost_estimate=cost,
        name="attend_far1",
    )(far1, gain, w_key, w_value, query_heads, bias, sums, atoms, w_out)
    mine, other, count = merged(stats, tile, "blk")
    return pl.pallas_call(
        functools.partial(forward_kernel, count=count),
        in_specs=[vmem] * 7,
        out_specs=hbm,
        out_shape=jax.ShapeDtypeStruct((tile, width), BF16),
        scratch_shapes=[pltpu.VMEM((tile, width), BF16), pltpu.SemaphoreType.DMA((2,))],
        compiler_params=params(12),
        cost_estimate=cost,
        name="feed_forward",
    )(after, mine, other, bn_gain.reshape(1, width), bn_shift.reshape(1, width), w_up, w_down)


def solution(mesh):
    rows = P(("grp", "blk"), None)
    placed = (rows, P(("grp", "blk"), None, None, None)) + (P(),) * 9


    return jax.shard_map(body, mesh=mesh, in_specs=placed, out_specs=rows, check_vma=False)
```
